32 devices in a mesh: replica: 2 (over core), fsdp: 16 (over z, y, x).
Axes of the slice: x: 2, y: 2, z: 4, core: 2. Of those that a mesh axis runs over, the one named last changes fastest.
Arguments:
- activations: bfloat16 [16384, 4096], P(('replica', 'fsdp')), may hold values from -6 to 6
- queries: bfloat16 [16384, 2048], P(('replica', 'fsdp')), may hold values from -60 to 60
- out_grad: bfloat16 [16384, 2048], P(('replica', 'fsdp')), may hold values from -6 to 6
- lengths: int32 [64], P(('replica', 'fsdp')), may hold values from 32 to 256
- norm_gain: float32 [4096], replicated, may hold values from 0.5 to 7
- key_master: float32 [4096, 512], P('fsdp'), may hold values from -0.09375 to 0.09375
- value_master: float32 [4096, 512], P('fsdp'), may hold values from -0.09375 to 0.09375
Outputs:
- key_direction: float32 [4096, 512], P('fsdp')
- value_direction: float32 [4096, 512], P('fsdp')
The draws below stay inside these ranges and needn't reach their ends.
All inputs are finite; a program needn't handle non-finite values.
Results may differ from the reference program's by a relative error of at most 0.009.
The reference program's roundings to bfloat16 on the way (of `normed`, `attended`, `value_grad`, `score_grad` and `key_grad`) count: a program that leaves them out, or rounds other values in their place, can miss the bound.
Values may be sent and summed in bfloat16 or wider, within the bound.
A program may use at most 128 MiB of HBM per device.

```python
import jax
import jax.numpy as jnp
from jax import lax

D = 4096
HD = 128
KVH = 4
GROUP = 4
LEN = 256
KVW = 512
QW = 2048
SEQS = 64
TOKENS = 16384
N_FSDP = 16


def draw_queries(key, part):
    baseline = jax.random.truncated_normal(key, -4.0, 4.0, (TOKENS, QW), jnp.float32)
    return baseline.astype(jnp.bfloat16)


def draw_norm_gain(key, part):
    row_index = jnp.arange(D, dtype=jnp.int32)
    block_rows = D // N_FSDP
    whole_frac = row_index.astype(jnp.float32) / D
    block_frac = (row_index % block_rows).astype(jnp.float32) / block_rows
    rough = jax.random.uniform(jax.random.fold_in(key, 11), (D,), jnp.float32, 0.85, 1.15)
    ramp = jnp.exp(jnp.log(3.0) * (0.6 * whole_frac + 0.6 * block_frac))
    return (ramp * rough).astype(jnp.float32)


def with_ends(result, key, least, high):
    longest = result.shape.index(max(result.shape))
    spots = []
    for shift in (0, 1):
        where = [jax.random.randint(jax.random.fold_in(key, axis), (), 0, length) for axis, length in enumerate(result.shape)]
        where[longest] = (where[longest] + shift) % result.shape[longest]
        spots.append(tuple(where))
    return result.at[spots[0]].set(least).at[spots[1]].set(high)


def with_spikes(result, key, source, target, shards_of, factor):
    def block_of(dim):
        return (jnp.arange(result.shape[dim]) // (result.shape[dim] // shards_of)).reshape((-1,) + (1,) * (result.ndim - 1 - dim))

    one_side = jax.random.permutation(key, shards_of)[block_of(target)]
    other_side = (block_of(target) + shards_of // 2) % shards_of
    return jnp.where((block_of(source) == one_side) | (block_of(source) == other_side), factor * result, result)


def level_of(key, dims, split, least, largest):
    level = 1.0
    for position, blocks in split:
        steps = jax.random.uniform(jax.random.fold_in(jax.random.fold_in(key, 6), position), (blocks,), jnp.float32, least / len(split), largest / len(split))
        level = level * jnp.repeat(jnp.exp(steps), dims[position] // blocks).reshape((-1,) + (1,) * (len(dims) - 1 - position))
    return level


def bell_draw(stream_key, shape, spread, limit, cuts=(), kind=jnp.bfloat16):
    drawn = jax.random.normal(stream_key, shape, jnp.float32) * spread
    if len(cuts) > 0:
        drawn = level_of(stream_key, shape, cuts, -0.22, 0.18) * drawn
    return jnp.clip(drawn, min=-limit, max=limit).astype(kind)


def heavy_noise(rng, shape, deviation, most, cuts, heavy, held_as=jnp.bfloat16):
    result = deviation * jax.random.normal(rng, shape, jnp.float32)
    if cuts:
        result = result * level_of(rng, shape, cuts, -0.22, 0.18)
    return jnp.clip(with_spikes(result, jax.random.fold_in(rng, 3), *heavy), -most, most).astype(held_as)


def setup_inputs(seed: int = 0) -> dict:
    key_of = jax.random.split(jax.random.key(seed), 8)
    return {
        "activations": heavy_noise(key_of[0], (TOKENS, D), 1.0, 6.0, ((0, 32),), (0, 1, 32, 2.75)),
        "queries": draw_queries(jax.random.fold_in(key_of[7], 71), 0),
        "out_grad": bell_draw(key_of[2], (TOKENS, QW), 1.0, 6.0, ((0, 32),)),
        "lengths": with_ends(jax.random.randint(key_of[3], (SEQS,), LEN // 8, LEN + 1), jax.random.fold_in(key_of[3], 1), LEN // 8, LEN).astype(jnp.int32),
        "norm_gain": draw_norm_gain(jax.random.fold_in(key_of[7], 71), 0),
        "key_master": bell_draw(key_of[5], (D, KVW), D ** -0.5, 0.09375, ((0, 16),), jnp.float32),
        "value_master": bell_draw(key_of[6], (D, KVW), D ** -0.5, 0.09375, ((0, 16),), jnp.float32),
    }


def attend(query_seq, key_seq, value_seq, grad_seq, length):
    scale_factor = 1.0 / HD ** 0.5
    positions = jnp.arange(LEN, dtype=jnp.int32)
    allowed = (positions[None, :] <= positions[:, None]) & (positions[None, :] < length)
    query_float = query_seq.astype(jnp.float32).reshape(LEN, KVH, GROUP, HD)
    key_float = key_seq.astype(jnp.float32).reshape(LEN, KVH, HD)
    value_float = value_seq.astype(jnp.float32).reshape(LEN, KVH, HD)
    scores = jnp.einsum('qhgd,khd->hgqk', query_float, key_float) * scale_factor
    scores = jnp.where(allowed[None, None], scores, jnp.float32(-1e+30))
    row_peak = lax.optimization_barrier(jnp.max(scores, axis=-1, keepdims=True))
    exponent = jnp.exp(scores - row_peak)
    probs = exponent / lax.optimization_barrier(jnp.sum(exponent, axis=-1, keepdims=True))
    probs_low = lax.optimization_barrier(probs.astype(jnp.bfloat16))
    probs_back = probs_low.astype(jnp.float32)
    attended = jnp.einsum('hgqk,khd->qhgd', probs_back, value_float).astype(jnp.bfloat16)
    attended = lax.optimization_barrier(attended).astype(jnp.float32)
    live_rows = (positions < length).astype(jnp.float32)
    grad_float = grad_seq.astype(jnp.float32).reshape(LEN, KVH, GROUP, HD) * live_rows[:, None, None, None]
    row_delta = jnp.transpose(lax.optimization_barrier(jnp.sum(grad_float * attended, axis=-1)), (1, 2, 0))[..., None]
    value_grad = jnp.einsum('hgqk,qhgd->khd', probs_back, grad_float).astype(jnp.bfloat16)
    prob_grad = jnp.einsum('qhgd,khd->hgqk', grad_float, value_float)
    score_grad = lax.optimization_barrier((probs * (prob_grad - row_delta)).astype(jnp.bfloat16))
    key_grad = (jnp.einsum('hgqk,qhgd->khd', score_grad.astype(jnp.float32), query_float) * scale_factor).astype(jnp.bfloat16)
    return (key_grad.reshape(LEN, KVH * HD), value_grad.reshape(LEN, KVH * HD))

def reference(activations, queries, out_grad, lengths, norm_gain, key_master, value_master):
    act_float = activations.astype(jnp.float32)
    inverse = lax.rsqrt(lax.optimization_barrier(jnp.mean(act_float * act_float, axis=-1, keepdims=True)) + 1e-05)
    normed = (act_float * inverse * norm_gain[None, :]).astype(jnp.bfloat16)
    key_proj = jnp.dot(normed, key_master.astype(jnp.bfloat16), preferred_element_type=jnp.float32).astype(jnp.bfloat16)
    value_proj = jnp.dot(normed, value_master.astype(jnp.bfloat16), preferred_element_type=jnp.float32).astype(jnp.bfloat16)
    width = KVH * HD
    qwidth = KVH * GROUP * HD

    def one_seq(packed):
        return attend(packed[0], packed[1], packed[2], packed[3], packed[4])
    key_grad, value_grad = lax.map(one_seq, (queries.reshape(SEQS, LEN, qwidth), key_proj.reshape(SEQS, LEN, width), value_proj.reshape(SEQS, LEN, width), out_grad.reshape(SEQS, LEN, qwidth), lengths))
    key_grad = key_grad.reshape(TOKENS, width)
    value_grad = value_grad.reshape(TOKENS, width)
    key_weight_grad = jnp.dot(normed.T, key_grad, preferred_element_type=jnp.float32)
    value_weight_grad = jnp.dot(normed.T, value_grad, preferred_element_type=jnp.float32)
    total_sq = jnp.sum(key_weight_grad * key_weight_grad) + jnp.sum(value_weight_grad * value_weight_grad)
    unit_scale = jnp.sqrt(jnp.float32(2 * D * width)) / jnp.sqrt(total_sq + 1e-06)
    return (unit_scale * key_weight_grad, unit_scale * value_weight_grad)
```

```python
import functools

import jax
import jax.numpy as jnp
from jax import lax
from jax.experimental import pallas as pl
from jax.experimental.pallas import tpu as pltpu
from jax.sharding import PartitionSpec as P

HD = 128
LEN = 256
MESH = pl.DeviceIdType.MESH
F32 = jnp.float32
BF16 = jnp.bfloat16


def factor_chips(mesh):
    total = mesh.shape["fsdp"]
    axis = mesh.axis_names.index("fsdp")
    line = mesh.devices.swapaxes(0, axis).reshape(total, -1)[:, 0]
    coords = [tuple(getattr(d, "coords", ())) for d in line]
    extents = []
    step = total
    if all(len(c) == 3 for c in coords):
        while step > 1:
            found = None
            for axis3 in range(3):
                count = len({c[axis3] for c in coords[:step]})
                if count > 1 and step % count == 0:
                    inner = step // count
                    if all(len({coords[k * inner + i][axis3] for i in range(inner)}) == 1 for k in range(count)):
                        found = (count, inner)
            if found is None:
                break
            extents.append(found[0])
            step = found[1]
    if step > 1:
        extents = [total]
    while len(extents) < 3:
        extents.append(1)
    if len(extents) > 3:
        extents = [total, 1, 1]
    return tuple(extents)


class Place:
    def __init__(self, dims):
        self.n0, n1, n2 = dims
        self.core = lax.axis_index("replica")
        self.me = lax.axis_index("fsdp")
        self.plane = n1 * n2
        self.a = self.me // self.plane
        b = (self.me // n2) % n1
        c = self.me % n2
        self.b, self.c = b, c
        swap = self.core if n1 == n2 else 0
        self.nf, self.ns = n2, n1
        self.stride_f = 1 + swap * (n2 - 1)
        self.stride_s = n2 - swap * (n2 - 1)
        self.f = c + swap * (b - c)
        self.s = b + swap * (c - b)

    def block(self, ja, kf, ks):
        a = lax.rem(self.a + ja, self.n0)
        f = lax.rem(self.f + kf, self.nf)
        s = lax.rem(self.s + ks, self.ns)
        return a * self.plane + f * self.stride_f + s * self.stride_s


def loop(lower, upper, body):
    def step(i, carry):
        body(i)
        return carry

    if upper > lower:
        lax.fori_loop(lower, upper, step, 0)


def gather_kernel(
    dims, act_hbm, gain_ref, own_ref, kv_ref, xn_ref, act, weights, acc,
    act_sem, send_sem, recv_sem, pass_sem, peer_sem,
):
    at = Place(dims)
    n = weights.shape[1]
    half = at.core
    other = 1 - at.core
    tokens = act.shape[0]
    rows = own_ref.shape[1]
    fetch = pltpu.make_async_copy(act_hbm, act, act_sem)

    def to_chip(src, piece, dest, slot):
        return pltpu.make_async_remote_copy(
            src_ref=src, dst_ref=weights.at[half, piece], send_sem=send_sem.at[slot],
            recv_sem=recv_sem.at[piece], device_id={"replica": half, "fsdp": dest}, device_id_type=MESH,
        )

    def to_peer(piece):
        return pltpu.make_async_remote_copy(
            src_ref=weights.at[half, piece], dst_ref=weights.at[half, piece], send_sem=pass_sem.at[piece],
            recv_sem=peer_sem.at[piece], device_id={"replica": other, "fsdp": at.me}, device_id_type=MESH,
        )

    def from_peer(piece):
        return pltpu.make_async_remote_copy(
            src_ref=weights.at[other, piece], dst_ref=weights.at[other, piece], send_sem=pass_sem.at[piece],
            recv_sem=peer_sem.at[piece], device_id={"replica": other, "fsdp": at.me}, device_id_type=MESH,
        )

    base_f = at.n0 - 1
    base_s = base_f + at.n0 * (at.nf - 1)
    per_s = at.nf * (at.ns - 1)

    def forward_f(src, piece, j):
        loop(1, at.nf, lambda k: to_chip(
            src, piece, at.block(0, k, 0), base_f + j * (at.nf - 1) + k - 1).start())

    def forward_s(src, piece, j, kf):
        loop(1, at.ns, lambda k: to_chip(
            src, piece, at.block(0, 0, k), base_s + j * per_s + kf * (at.ns - 1) + k - 1).start())

    mine = own_ref.at[half]
    loop(1, at.n0, lambda j: to_chip(mine, at.me, at.block(j, 0, 0), j - 1).start())
    forward_f(mine, at.me, 0)
    forward_s(mine, at.me, 0, 0)
    fetch.start()
    acc[...] = jnp.zeros_like(acc)
    fetch.wait()

    chunk = 32

    def norm(i):
        part = act[pl.ds(pl.multiple_of(i * chunk, chunk), chunk), :].astype(F32)
        inverse = lax.rsqrt(jnp.mean(part * part, axis=-1, keepdims=True) + 1e-05)
        normed = (part * inverse * gain_ref[...]).astype(BF16)
        for p in range(n):
            xn_ref[p, pl.ds(pl.multiple_of(i * chunk, chunk), chunk), :] = normed[:, p * rows:(p + 1) * rows]

    loop(0, tokens // chunk, norm)

    def multiply(which, piece):
        acc[which] += jnp.dot(xn_ref[piece], weights[which, piece], preferred_element_type=F32)

    def arrive(piece, j, kf, kind):
        to_chip(mine, piece, at.me, 0).wait_recv()
        src = weights.at[half, piece]
        if kind == 0:
            forward_f(src, piece, j)
        if kind <= 1:
            forward_s(src, piece, j, kf)
        to_peer(piece).start()
        multiply(half, piece)

    for which in range(2):
        acc[which] += jnp.dot(xn_ref[at.me], own_ref[which], preferred_element_type=F32)
    for t in range(at.n0 + 2):
        if 1 <= t < at.n0:
            arrive(at.block(at.n0 - t, 0, 0), t, 0, 0)
        j = t - 1
        if 0 <= j < at.n0:
            loop(1, at.nf, lambda k: arrive(at.block(at.n0 - j, k, 0), j, k, 1))
        j2 = t - 2
        if 0 <= j2 < at.n0:
            loop(0, at.nf * (at.ns - 1), lambda k: arrive(
                at.block(at.n0 - j2, k // (at.ns - 1), k % (at.ns - 1) + 1), j2, 0, 2))

    def close(k):
        piece = lax.rem(at.me + k, n)
        from_peer(piece).wait_recv()
        multiply(other, piece)

    loop(1, n, close)
    loop(0, 2, lambda w: kv_ref.__setitem__(w, acc[w].astype(BF16)))
    loop(0, n - 1, lambda k: to_chip(mine, at.me, at.me, k).wait_send())
    loop(1, n, lambda k: to_peer(lax.rem(at.me + k, n)).wait_send())


def attend_kernel(group, lengths_ref, q_ref, g_ref, kv_ref, out_ref):
    seq = pl.program_id(0)
    length = lengths_ref[seq]
    scale = 1.0 / HD**0.5
    key_pos = lax.broadcasted_iota(jnp.int32, (LEN, LEN), 0)
    query_pos = lax.broadcasted_iota(jnp.int32, (LEN, LEN), 1)
    allowed = (key_pos <= query_pos) & (key_pos < length)
    live = lax.broadcasted_iota(jnp.int32, (LEN, HD), 0) < length
    key = kv_ref[0]
    value = kv_ref[1]
    last = (((1,), (1,)), ((), ()))
    key_grad = jnp.zeros((LEN, HD), F32)
    value_grad = jnp.zeros((LEN, HD), F32)
    for head in range(group):
        query = q_ref[:, head * HD:(head + 1) * HD]
        grad = jnp.where(live, g_ref[:, head * HD:(head + 1) * HD].astype(F32), 0.0)
        grad_low = grad.astype(BF16)
        grad_flip = grad.T
        scores = lax.dot_general(key, query, last, preferred_element_type=F32) * scale
        scores = jnp.where(allowed, scores, -1e30)
        peak = jnp.max(scores, axis=0, keepdims=True)
        exponent = jnp.exp(scores - peak)
        probs = exponent / jnp.sum(exponent, axis=0, keepdims=True)
        probs_low = probs.astype(BF16)
        attended = lax.dot_general(
            value, probs_low, (((0,), (0,)), ((), ())), preferred_element_type=F32).astype(BF16).astype(F32)
        delta = jnp.sum(grad_flip * attended, axis=0, keepdims=True)
        value_grad += jnp.dot(probs_low, grad_low, preferred_element_type=F32)
        prob_grad = lax.dot_general(value, grad_low, last, preferred_element_type=F32)
        score_grad = (probs * (prob_grad - delta)).astype(BF16)
        key_grad += jnp.dot(score_grad, query, preferred_element_type=F32)
    out_ref[0] = (key_grad * scale).astype(BF16)
    out_ref[1] = value_grad.astype(BF16)


def scatter_kernel(
    dims, count, xn_ref, dkv_ref, key_ref, value_ref, part, give, take, sendbuf, recvbuf, endbuf, sums,
    give_sem, take_sem, send_sem, recv_sem, end_send, end_recv, sum_send, sum_recv,
):
    at = Place(dims)
    n = part.shape[0]
    half = at.core
    other = 1 - at.core

    def to_peer(p):
        return pltpu.make_async_remote_copy(
            src_ref=give.at[p], dst_ref=take.at[p], send_sem=give_sem.at[p], recv_sem=take_sem.at[p],
            device_id={"replica": other, "fsdp": at.me}, device_id_type=MESH,
        )

    def to_chip(p, slot, dest):
        return pltpu.make_async_remote_copy(
            src_ref=sendbuf.at[p], dst_ref=recvbuf.at[slot], send_sem=send_sem.at[p],
            recv_sem=recv_sem.at[slot], device_id={"replica": half, "fsdp": dest}, device_id_type=MESH,
        )

    def compute(p):
        full = (((0,), (0,)), ((), ()))
        give[p] = lax.dot_general(
            xn_ref[p], dkv_ref[other], full, preferred_element_type=F32).astype(BF16)
        part[p] = lax.dot_general(xn_ref[p], dkv_ref[half], full, preferred_element_type=F32)
        to_peer(p).start()

    ahead = at.n0 * at.nf * (at.ns - 1)
    deep = ahead + at.n0 * (at.nf - 1)

    def slot_s(ja, kf, ks):
        a = lax.rem(at.a + ja, at.n0)
        f = lax.rem(at.f + kf, at.nf)
        return (ks - 1) * at.n0 * at.nf + a * at.nf + f

    def slot_f(ja, kf):
        return ahead + (kf - 1) * at.n0 + lax.rem(at.a + ja, at.n0)

    def slot_z(ja):
        return deep + ja - 1

    def landed(slot):
        to_chip(0, slot, at.me).wait_recv()
        return recvbuf[slot].astype(F32)

    def paired(p):
        to_peer(p).wait_recv()
        return part[p] + take[p].astype(F32)

    def gathered_s(ja, kf, p):
        total = paired(p)
        for ks in range(1, at.ns):
            total += landed(slot_s(ja, kf, ks))
        return total

    def gathered_f(ja, p):
        total = gathered_s(ja, 0, p)
        for kf in range(1, at.nf):
            total += landed(slot_f(ja, kf))
        return total

    def later(i):
        return lax.rem(i + 1, at.n0)

    def send_s(ja, kf, ks):
        p = at.block(ja, kf, ks)
        sendbuf[p] = paired(p).astype(BF16)
        to_chip(p, slot_s(ja, kf, ks), at.block(0, 0, ks)).start()

    def send_f(ja, kf):
        p = at.block(ja, kf, 0)
        sendbuf[p] = gathered_s(ja, kf, p).astype(BF16)
        to_chip(p, slot_f(ja, kf), at.block(0, kf, 0)).start()

    def send_z(ja):
        p = at.block(ja, 0, 0)
        sendbuf[p] = gathered_f(ja, p).astype(BF16)
        to_chip(p, slot_z(ja), p).start()

    ns1, nf1, n0 = at.ns - 1, at.nf - 1, at.n0
    loop(0, n0 * nf1 * ns1, lambda i: compute(
        at.block(later(i // (nf1 * ns1)), i // ns1 % nf1 + 1, i % ns1 + 1)))
    loop(0, n0 * nf1 * ns1, lambda i: send_s(
        later(i // (nf1 * ns1)), i // ns1 % nf1 + 1, i % ns1 + 1))
    loop(0, n0 * ns1, lambda i: compute(at.block(later(i // ns1), 0, i % ns1 + 1)))
    loop(0, n0 * nf1, lambda i: compute(at.block(later(i // nf1), i % nf1 + 1, 0)))
    loop(0, n0, lambda i: compute(at.block(i, 0, 0)))
    loop(0, n0 * ns1, lambda i: send_s(later(i // ns1), 0, i % ns1 + 1))
    loop(0, n0 * nf1, lambda i: send_f(later(i // nf1), i % nf1 + 1))
    loop(1, n0, send_z)
    owned = gathered_f(0, at.me)
    for ja in range(1, n0):
        owned += landed(slot_z(ja))
    endbuf[0] = owned.astype(BF16)

    trade = pltpu.make_async_remote_copy(
        src_ref=endbuf.at[0], dst_ref=endbuf.at[1], send_sem=end_send, recv_sem=end_recv,
        device_id={"replica": other, "fsdp": at.me}, device_id_type=MESH,
    )
    squares = jnp.sum(owned * owned)
    total = jnp.full((8, 128), squares, F32)
    n1, n2 = dims[1], dims[2]
    base = 0
    started = []
    for level, (size, digit, stride) in enumerate(
        ((n0, at.a, n1 * n2), (n1, at.b, n2), (n2, at.c, 1), (2, at.core, 0))
    ):
        if size > 1:
            sums[base + digit] = total
            for k in range(1, size):
                to = lax.rem(digit + k, size)
                if level == 3:
                    target = {"replica": other, "fsdp": at.me}
                else:
                    target = {"replica": half, "fsdp": at.me + (to - digit) * stride}
                copy = pltpu.make_async_remote_copy(
                    src_ref=sums.at[base + digit], dst_ref=sums.at[base + digit],
                    send_sem=sum_send.at[base + k], recv_sem=sum_recv.at[base + digit],
                    device_id=target, device_id_type=MESH,
                )
                copy.start()
                started.append(copy)
            if level == 0:
                trade.start()
            for k in range(1, size):
                came = lax.rem(digit + k, size)
                pltpu.make_async_remote_copy(
                    src_ref=sums.at[base + came], dst_ref=sums.at[base + came],
                    send_sem=sum_send.at[base + k], recv_sem=sum_recv.at[base + came],
                    device_id={"replica": other, "fsdp": at.me}, device_id_type=MESH,
                ).wait_recv()
            total = sums[base]
            for k in range(1, size):
                total += sums[base + k]
        elif level == 0:
            trade.start()
        base += size
    unit = jnp.sqrt(F32(count)) / jnp.sqrt(total + 1e-06)
    unit = unit[0:1, 0:1]
    trade.wait_recv()

    @pl.when(at.core == 0)
    def _():
        key_ref[...] = unit * endbuf[0].astype(F32)
        value_ref[...] = unit * endbuf[1].astype(F32)

    @pl.when(at.core == 1)
    def _():
        key_ref[...] = unit * endbuf[1].astype(F32)
        value_ref[...] = unit * endbuf[0].astype(F32)

    trade.wait_send()
    for copy in started:
        copy.wait_send()
    loop(0, n, lambda p: to_peer(p).wait_send())
    loop(1, n, lambda k: to_chip(lax.rem(at.me + k, n), 0, at.me).wait_send())


VMEM = pl.BlockSpec(memory_space=pltpu.VMEM)
LIMIT = 60 * 1024 * 1024


def local(dims, activations, queries, out_grad, lengths, norm_gain, key_master, value_master):
    tokens, features = activations.shape
    rows, width = key_master.shape
    n = features // rows
    qwidth = queries.shape[1]
    group = qwidth // width
    heads = width // HD
    seqs = lengths.shape[0]
    own = jnp.stack([key_master.astype(BF16), value_master.astype(BF16)])
    dma = pltpu.SemaphoreType.DMA
    kv, xn = pl.pallas_call(
        functools.partial(gather_kernel, dims),
        out_shape=(
            jax.ShapeDtypeStruct((2, tokens, width), BF16),
            jax.ShapeDtypeStruct((n, tokens, rows), BF16),
        ),
        in_specs=[pl.BlockSpec(memory_space=pl.ANY), VMEM, VMEM],
        out_specs=(VMEM, VMEM),
        scratch_shapes=[
            pltpu.VMEM((tokens, features), BF16),
            pltpu.VMEM((2, n, rows, width), BF16),
            pltpu.VMEM((2, tokens, width), F32),
            dma, dma((n,)), dma((n,)), dma((n,)), dma((n,)),
        ],
        compiler_params=pltpu.CompilerParams(has_side_effects=True, vmem_limit_bytes=LIMIT),
    )(activations, norm_gain.reshape(1, features), own)
    dkv = pl.pallas_call(
        functools.partial(attend_kernel, group),
        out_shape=jax.ShapeDtypeStruct((2, tokens, width), BF16),
        grid=(seqs, heads),
        in_specs=[
            pl.BlockSpec(memory_space=pltpu.SMEM),
            pl.BlockSpec((LEN, group * HD), lambda s, h: (s, h)),
            pl.BlockSpec((LEN, group * HD), lambda s, h: (s, h)),
            pl.BlockSpec((2, LEN, HD), lambda s, h: (0, s, h)),
        ],
        out_specs=pl.BlockSpec((2, LEN, HD), lambda s, h: (0, s, h)),
    )(lengths, queries, out_grad, kv)
    shape = jax.ShapeDtypeStruct((rows, width), F32)
    return pl.pallas_call(
        functools.partial(scatter_kernel, dims, 2 * features * width),
        out_shape=(shape, shape),
        in_specs=[VMEM, VMEM],
        out_specs=(VMEM, VMEM),
        scratch_shapes=[
            pltpu.VMEM((n, rows, width), F32),
            pltpu.VMEM((n, rows, width), BF16),
            pltpu.VMEM((n, rows, width), BF16),
            pltpu.VMEM((n, rows, width), BF16),
            pltpu.VMEM((n, rows, width), BF16),
            pltpu.VMEM((2, rows, width), BF16),
            pltpu.VMEM((sum(dims) + 2, 8, 128), F32),
            dma((n,)), dma((n,)), dma((n,)), dma((n,)), dma, dma,
            dma((sum(dims) + 2,)), dma((sum(dims) + 2,)),
        ],
        compiler_params=pltpu.CompilerParams(has_side_effects=True, vmem_limit_bytes=LIMIT),
    )(xn, dkv)


def solution(mesh):
    in_specs = (
        P(("replica", "fsdp"), None),
        P(("replica", "fsdp"), None),
        P(("replica", "fsdp"), None),
        P(("replica", "fsdp")),
        P(),
        P("fsdp", None),
        P("fsdp", None),
    )
    out_specs = (P("fsdp", None), P("fsdp", None))
    body = functools.partial(local, factor_chips(mesh))
    return jax.shard_map(body, mesh=mesh, in_specs=in_specs, out_specs=out_specs, check_vma=False)
```

```python
import functools

import jax
import jax.numpy as jnp
from jax import lax
from jax.experimental import pallas as pl
from jax.experimental.pallas import tpu as pltpu
from jax.sharding import PartitionSpec as P

HD = 128
LEN = 256
MESH = pl.DeviceIdType.MESH
F32 = jnp.float32
BF16 = jnp.bfloat16


def factor_chips(mesh):
    total = mesh.shape["fsdp"]
    axis = mesh.axis_names.index("fsdp")
    line = mesh.devices.swapaxes(0, axis).reshape(total, -1)[:, 0]
    coords = [tuple(getattr(d, "coords", ())) for d in line]
    extents = []
    step = total
    if all(len(c) == 3 for c in coords):
        while step > 1:
            found = None
            for axis3 in range(3):
                count = len({c[axis3] for c in coords[:step]})
                if count > 1 and step % count == 0:
                    inner = step // count
                    if all(len({coords[k * inner + i][axis3] for i in range(inner)}) == 1 for k in range(count)):
                        found = (count, inner)
            if found is None:
                break
            extents.append(found[0])
            step = found[1]
    if step > 1:
        extents = [total]
    while len(extents) < 3:
        extents.append(1)
    if len(extents) > 3:
        extents = [total, 1, 1]
    return tuple(extents)


class Place:
    def __init__(self, dims):
        self.n0, n1, n2 = dims
        self.core = lax.axis_index("replica")
        self.me = lax.axis_index("fsdp")
        self.plane = n1 * n2
        self.a = self.me // self.plane
        b = (self.me // n2) % n1
        c = self.me % n2
        self.b, self.c = b, c
        swap = self.core if n1 == n2 else 0
        self.nf, self.ns = n2, n1
        self.stride_f = 1 + swap * (n2 - 1)
        self.stride_s = n2 - swap * (n2 - 1)
        self.f = c + swap * (b - c)
        self.s = b + swap * (c - b)

    def block(self, ja, kf, ks):
        a = lax.rem(self.a + ja, self.n0)
        f = lax.rem(self.f + kf, self.nf)
        s = lax.rem(self.s + ks, self.ns)
        return a * self.plane + f * self.stride_f + s * self.stride_s


def loop(lower, upper, body):
    def step(i, carry):
        body(i)
        return carry

    if upper > lower:
        lax.fori_loop(lower, upper, step, 0)


def gather_kernel(
    dims, act_hbm, gain_ref, own_ref, kv_ref, xn_ref, act, weights, acc,
    act_sem, send_sem, recv_sem, pass_sem, peer_sem, line_sem,
):
    at = Place(dims)
    n = weights.shape[1]
    half = at.core
    other = 1 - at.core
    tokens = act.shape[0]
    rows = own_ref.shape[1]
    fetch = pltpu.make_async_copy(act_hbm, act, act_sem)

    def to_chip(src, piece, dest, slot):
        return pltpu.make_async_remote_copy(
            src_ref=src, dst_ref=weights.at[half, piece], send_sem=send_sem.at[slot],
            recv_sem=recv_sem.at[piece], device_id={"replica": half, "fsdp": dest}, device_id_type=MESH,
        )

    def to_peer(piece):
        return pltpu.make_async_remote_copy(
            src_ref=weights.at[half, piece], dst_ref=weights.at[half, piece], send_sem=pass_sem.at[piece],
            recv_sem=peer_sem.at[piece], device_id={"replica": other, "fsdp": at.me}, device_id_type=MESH,
        )

    def from_peer(piece):
        return pltpu.make_async_remote_copy(
            src_ref=weights.at[other, piece], dst_ref=weights.at[other, piece], send_sem=pass_sem.at[piece],
            recv_sem=peer_sem.at[piece], device_id={"replica": other, "fsdp": at.me}, device_id_type=MESH,
        )

    def along(src, piece, a, slot):
        dest = at.me + (a - at.a) * at.plane
        return pltpu.make_async_remote_copy(
            src_ref=src, dst_ref=weights.at[half, piece], send_sem=line_sem.at[slot],
            recv_sem=recv_sem.at[piece], device_id={"replica": half, "fsdp": dest}, device_id_type=MESH,
        )

    n0, a = at.n0, at.a
    base_f = 0
    base_s = base_f + at.n0 * (at.nf - 1)
    per_s = at.nf * (at.ns - 1)

    def forward_f(src, piece, j):
        loop(1, at.nf, lambda k: to_chip(
            src, piece, at.block(0, k, 0), base_f + j * (at.nf - 1) + k - 1).start())

    def forward_s(src, piece, j, kf):
        loop(1, at.ns, lambda k: to_chip(
            src, piece, at.block(0, 0, k), base_s + j * per_s + kf * (at.ns - 1) + k - 1).start())

    mine = own_ref.at[half]
    pl.when(a + 1 < n0)(lambda: along(mine, at.me, a + 1, n0).start())
    pl.when(a > 0)(lambda: along(mine, at.me, a - 1, n0 + 1).start())
    forward_f(mine, at.me, 0)
    forward_s(mine, at.me, 0, 0)
    fetch.start()
    acc[...] = jnp.zeros_like(acc)
    fetch.wait()

    chunk = 32

    def norm(i):
        part = act[pl.ds(pl.multiple_of(i * chunk, chunk), chunk), :].astype(F32)
        inverse = lax.rsqrt(jnp.mean(part * part, axis=-1, keepdims=True) + 1e-05)
        normed = (part * inverse * gain_ref[...]).astype(BF16)
        for p in range(n):
            xn_ref[p, pl.ds(pl.multiple_of(i * chunk, chunk), chunk), :] = normed[:, p * rows:(p + 1) * rows]

    loop(0, tokens // chunk, norm)

    def multiply(which, piece):
        acc[which] += jnp.dot(xn_ref[piece], weights[which, piece], preferred_element_type=F32)

    def arrive(piece, j, kf):
        to_chip(mine, piece, at.me, 0).wait_recv()
        if kf is not None:
            forward_s(weights.at[half, piece], piece, j, kf)
        to_peer(piece).start()
        multiply(half, piece)

    for which in range(2):
        acc[which] += jnp.dot(xn_ref[at.me], own_ref[which], preferred_element_type=F32)
    def first(step, away):
        piece = at.me + step * away * at.plane
        to_chip(mine, piece, at.me, 0).wait_recv()
        nearer = a - step
        pl.when((nearer >= 0) & (nearer < n0))(
            lambda: along(weights.at[half, piece], piece, nearer, a + step * away).start())
        src = weights.at[half, piece]
        j = lax.rem(n0 + step * away, n0)
        forward_f(src, piece, j)
        forward_s(src, piece, j, 0)
        to_peer(piece).start()
        multiply(half, piece)

    def second(step, away):
        j = lax.rem(n0 + step * away, n0)
        loop(1, at.nf, lambda k: arrive(at.block(j, k, 0), j, k))

    def third(step, away):
        j = lax.rem(n0 + step * away, n0)
        loop(0, at.nf * (at.ns - 1), lambda k: arrive(
            at.block(j, k // (at.ns - 1), k % (at.ns - 1) + 1), j, None))

    for t in range(n0 + 2):
        for lag, work in enumerate((first, second, third)):
            away = t - lag
            if away == 0 and lag > 0:
                work(1, 0)
            elif 0 < away < n0:
                pl.when(a - away >= 0)(lambda: work(-1, away))
                pl.when(a + away < n0)(lambda: work(1, away))

    def close(k):
        piece = lax.rem(at.me + k, n)
        from_peer(piece).wait_recv()
        multiply(other, piece)

    loop(1, n, close)
    loop(0, 2, lambda w: kv_ref.__setitem__(w, acc[w].astype(BF16)))
    loop(0, n - n0, lambda k: to_chip(mine, at.me, at.me, k).wait_send())
    pl.when(a + 1 < n0)(lambda: along(mine, at.me, a, n0).wait_send())
    pl.when(a > 0)(lambda: along(mine, at.me, a, n0 + 1).wait_send())
    for k in range(n0):
        pl.when(((k < a) & (a + 1 < n0)) | ((k > a) & (a > 0)))(
            lambda: along(mine, at.me, a, k).wait_send())
    loop(1, n, lambda k: to_peer(lax.rem(at.me + k, n)).wait_send())


def attend_kernel(group, lengths_ref, q_ref, g_ref, kv_ref, out_ref):
    seq = pl.program_id(0)
    length = lengths_ref[seq]
    scale = 1.0 / HD**0.5
    key_pos = lax.broadcasted_iota(jnp.int32, (LEN, LEN), 0)
    query_pos = lax.broadcasted_iota(jnp.int32, (LEN, LEN), 1)
    allowed = (key_pos <= query_pos) & (key_pos < length)
    live = lax.broadcasted_iota(jnp.int32, (LEN, HD), 0) < length
    key = kv_ref[0]
    value = kv_ref[1]
    last = (((1,), (1,)), ((), ()))
    key_grad = jnp.zeros((LEN, HD), F32)
    value_grad = jnp.zeros((LEN, HD), F32)
    for head in range(group):
        query = q_ref[:, head * HD:(head + 1) * HD]
        grad = jnp.where(live, g_ref[:, head * HD:(head + 1) * HD].astype(F32), 0.0)
        grad_low = grad.astype(BF16)
        grad_flip = grad.T
        scores = lax.dot_general(key, query, last, preferred_element_type=F32) * scale
        scores = jnp.where(allowed, scores, -1e30)
        peak = jnp.max(scores, axis=0, keepdims=True)
        exponent = jnp.exp(scores - peak)
        probs = exponent / jnp.sum(exponent, axis=0, keepdims=True)
        probs_low = probs.astype(BF16)
        attended = lax.dot_general(
            value, probs_low, (((0,), (0,)), ((), ())), preferred_element_type=F32).astype(BF16).astype(F32)
        delta = jnp.sum(grad_flip * attended, axis=0, keepdims=True)
        value_grad += jnp.dot(probs_low, grad_low, preferred_element_type=F32)
        prob_grad = lax.dot_general(value, grad_low, last, preferred_element_type=F32)
        score_grad = (probs * (prob_grad - delta)).astype(BF16)
        key_grad += jnp.dot(score_grad, query, preferred_element_type=F32)
    out_ref[0] = (key_grad * scale).astype(BF16)
    out_ref[1] = value_grad.astype(BF16)


def scatter_kernel(
    dims, count, xn_ref, dkv_ref, both_ref, unit_ref, part, give, take, sendbuf, recvbuf, endbuf, sums,
    give_sem, take_sem, send_sem, recv_sem, end_send, end_recv, sum_send, sum_recv,
):
    at = Place(dims)
    n = part.shape[0]
    half = at.core
    other = 1 - at.core

    def to_peer(p):
        return pltpu.make_async_remote_copy(
            src_ref=give.at[p], dst_ref=take.at[p], send_sem=give_sem.at[p], recv_sem=take_sem.at[p],
            device_id={"replica": other, "fsdp": at.me}, device_id_type=MESH,
        )

    def to_chip(p, slot, dest):
        return pltpu.make_async_remote_copy(
            src_ref=sendbuf.at[p], dst_ref=recvbuf.at[slot], send_sem=send_sem.at[p],
            recv_sem=recv_sem.at[slot], device_id={"replica": half, "fsdp": dest}, device_id_type=MESH,
        )

    def compute(p):
        full = (((0,), (0,)), ((), ()))
        give[p] = lax.dot_general(
            xn_ref[p], dkv_ref[other], full, preferred_element_type=F32).astype(BF16)
        part[p] = lax.dot_general(xn_ref[p], dkv_ref[half], full, preferred_element_type=F32)
        to_peer(p).start()

    ahead = at.n0 * at.nf * (at.ns - 1)
    deep = ahead + at.n0 * (at.nf - 1)

    def slot_s(ja, kf, ks):
        a = lax.rem(at.a + ja, at.n0)
        f = lax.rem(at.f + kf, at.nf)
        return (ks - 1) * at.n0 * at.nf + a * at.nf + f

    def slot_f(ja, kf):
        return ahead + (kf - 1) * at.n0 + lax.rem(at.a + ja, at.n0)

    def slot_z(ja):
        return deep + ja - 1

    def landed(slot):
        to_chip(0, slot, at.me).wait_recv()
        return recvbuf[slot].astype(F32)

    def paired(p):
        to_peer(p).wait_recv()
        return part[p] + take[p].astype(F32)

    def gathered_s(ja, kf, p):
        total = paired(p)
        for ks in range(1, at.ns):
            total += landed(slot_s(ja, kf, ks))
        return total

    def gathered_f(ja, p):
        total = gathered_s(ja, 0, p)
        for kf in range(1, at.nf):
            total += landed(slot_f(ja, kf))
        return total

    def later(i):
        return lax.rem(i + 1, at.n0)

    def send_s(ja, kf, ks):
        p = at.block(ja, kf, ks)
        sendbuf[p] = paired(p).astype(BF16)
        to_chip(p, slot_s(ja, kf, ks), at.block(0, 0, ks)).start()

    def send_f(ja, kf):
        p = at.block(ja, kf, 0)
        sendbuf[p] = gathered_s(ja, kf, p).astype(BF16)
        to_chip(p, slot_f(ja, kf), at.block(0, kf, 0)).start()

    def send_z(ja):
        p = at.block(ja, 0, 0)
        sendbuf[p] = gathered_f(ja, p).astype(BF16)
        to_chip(p, slot_z(ja), p).start()

    ns1, nf1, n0 = at.ns - 1, at.nf - 1, at.n0
    loop(0, n0 * nf1 * ns1, lambda i: compute(
        at.block(later(i // (nf1 * ns1)), i // ns1 % nf1 + 1, i % ns1 + 1)))
    loop(0, n0 * nf1 * ns1, lambda i: send_s(
        later(i // (nf1 * ns1)), i // ns1 % nf1 + 1, i % ns1 + 1))
    loop(0, n0 * ns1, lambda i: compute(at.block(later(i // ns1), 0, i % ns1 + 1)))
    loop(0, n0 * nf1, lambda i: compute(at.block(later(i // nf1), i % nf1 + 1, 0)))
    loop(0, n0, lambda i: compute(at.block(i, 0, 0)))
    loop(0, n0 * ns1, lambda i: send_s(later(i // ns1), 0, i % ns1 + 1))
    loop(0, n0 * nf1, lambda i: send_f(later(i // nf1), i % nf1 + 1))
    loop(1, n0, send_z)
    owned = gathered_f(0, at.me)
    for ja in range(1, n0):
        owned += landed(slot_z(ja))
    endbuf[0] = owned.astype(BF16)

    trade = pltpu.make_async_remote_copy(
        src_ref=endbuf.at[0], dst_ref=endbuf.at[1], send_sem=end_send, recv_sem=end_recv,
        device_id={"replica": other, "fsdp": at.me}, device_id_type=MESH,
    )
    squares = jnp.sum(owned * owned)
    total = jnp.full((8, 128), squares, F32)
    n1, n2 = dims[1], dims[2]
    base = 0
    started = []
    for level, (size, digit, stride) in enumerate(
        ((n0, at.a, n1 * n2), (n1, at.b, n2), (n2, at.c, 1), (2, at.core, 0))
    ):
        if size > 1:
            sums[base + digit] = total
            for k in range(1, size):
                to = lax.rem(digit + k, size)
                if level == 3:
                    target = {"replica": other, "fsdp": at.me}
                else:
                    target = {"replica": half, "fsdp": at.me + (to - digit) * stride}
                copy = pltpu.make_async_remote_copy(
                    src_ref=sums.at[base + digit], dst_ref=sums.at[base + digit],
                    send_sem=sum_send.at[base + k], recv_sem=sum_recv.at[base + digit],
                    device_id=target, device_id_type=MESH,
                )
                copy.start()
                started.append(copy)
            if level == 0:
                trade.start()
            for k in range(1, size):
                came = lax.rem(digit + k, size)
                pltpu.make_async_remote_copy(
                    src_ref=sums.at[base + came], dst_ref=sums.at[base + came],
                    send_sem=sum_send.at[base + k], recv_sem=sum_recv.at[base + came],
                    device_id={"replica": other, "fsdp": at.me}, device_id_type=MESH,
                ).wait_recv()
            total = sums[base]
            for k in range(1, size):
                total += sums[base + k]
        elif level == 0:
            trade.start()
        base += size
    unit = jnp.sqrt(F32(count)) / jnp.sqrt(total + 1e-06)
    unit_ref[...] = unit
    both_ref[half] = endbuf[0]
    trade.wait_recv()
    both_ref[other] = endbuf[1]
    trade.wait_send()
    for copy in started:
        copy.wait_send()
    loop(0, n, lambda p: to_peer(p).wait_send())
    loop(1, n, lambda k: to_chip(lax.rem(at.me + k, n), 0, at.me).wait_send())


VMEM = pl.BlockSpec(memory_space=pltpu.VMEM)
LIMIT = 60 * 1024 * 1024


def local(dims, activations, queries, out_grad, lengths, norm_gain, key_master, value_master):
    tokens, features = activations.shape
    rows, width = key_master.shape
    n = features // rows
    qwidth = queries.shape[1]
    group = qwidth // width
    heads = width // HD
    seqs = lengths.shape[0]
    own = jnp.stack([key_master.astype(BF16), value_master.astype(BF16)])
    dma = pltpu.SemaphoreType.DMA
    kv, xn = pl.pallas_call(
        functools.partial(gather_kernel, dims),
        out_shape=(
            jax.ShapeDtypeStruct((2, tokens, width), BF16),
            jax.ShapeDtypeStruct((n, tokens, rows), BF16),
        ),
        in_specs=[pl.BlockSpec(memory_space=pl.ANY), VMEM, VMEM],
        out_specs=(VMEM, VMEM),
        scratch_shapes=[
            pltpu.VMEM((tokens, features), BF16),
            pltpu.VMEM((2, n, rows, width), BF16),
            pltpu.VMEM((2, tokens, width), F32),
            dma, dma((n,)), dma((n,)), dma((n,)), dma((n,)), dma((dims[0] + 2,)),
        ],
        compiler_params=pltpu.CompilerParams(has_side_effects=True, vmem_limit_bytes=LIMIT),
    )(activations, norm_gain.reshape(1, features), own)
    dkv = pl.pallas_call(
        functools.partial(attend_kernel, group),
        out_shape=jax.ShapeDtypeStruct((2, tokens, width), BF16),
        grid=(seqs, heads),
        in_specs=[
            pl.BlockSpec(memory_space=pltpu.SMEM),
            pl.BlockSpec((LEN, group * HD), lambda s, h: (s, h)),
            pl.BlockSpec((LEN, group * HD), lambda s, h: (s, h)),
            pl.BlockSpec((2, LEN, HD), lambda s, h: (0, s, h)),
        ],
        out_specs=pl.BlockSpec((2, LEN, HD), lambda s, h: (0, s, h)),
    )(lengths, queries, out_grad, kv)
    both, unit = pl.pallas_call(
        functools.partial(scatter_kernel, dims, 2 * features * width),
        out_shape=(jax.ShapeDtypeStruct((2, rows, width), BF16), jax.ShapeDtypeStruct((8, 128), F32)),
        in_specs=[VMEM, VMEM],
        out_specs=(VMEM, VMEM),
        scratch_shapes=[
            pltpu.VMEM((n, rows, width), F32),
            pltpu.VMEM((n, rows, width), BF16),
            pltpu.VMEM((n, rows, width), BF16),
            pltpu.VMEM((n, rows, width), BF16),
            pltpu.VMEM((n, rows, width), BF16),
            pltpu.VMEM((2, rows, width), BF16),
            pltpu.VMEM((sum(dims) + 2, 8, 128), F32),
            dma((n,)), dma((n,)), dma((n,)), dma((n,)), dma, dma,
            dma((sum(dims) + 2,)), dma((sum(dims) + 2,)),
        ],
        compiler_params=pltpu.CompilerParams(has_side_effects=True, vmem_limit_bytes=LIMIT),
    )(xn, dkv)
    scale = unit[0, 0]
    return scale * both[0].astype(F32), scale * both[1].astype(F32)


def solution(mesh):
    in_specs = (
        P(("replica", "fsdp"), None),
        P(("replica", "fsdp"), None),
        P(("replica", "fsdp"), None),
        P(("replica", "fsdp")),
        P(),
        P("fsdp", None),
        P("fsdp", None),
    )
    out_specs = (P("fsdp", None), P("fsdp", None))
    body = functools.partial(local, factor_chips(mesh))
    return jax.shard_map(body, mesh=mesh, in_specs=in_specs, out_specs=out_specs, check_vma=False)
```
